32 devices in a mesh: grp: 8 (over z, x), tp: 4 (over y, core).
Axes of the slice: x: 2, y: 2, z: 4, core: 2. Of those that a mesh axis runs over, the one named last changes fastest.
Arguments:
- q_nope: bfloat16 [512, 16384], P('grp', 'tp'), may hold values from -6 to 6
- q_rope: bfloat16 [512, 8192], P('grp', 'tp'), may hold values from -500 to 500
- w_uk: bfloat16 [128, 128, 512], P('tp'), may hold values from -0.5 to 0.5
- w_uv: bfloat16 [128, 512, 128], P('tp'), may hold values from -1 to 1
- prefix_latent: bfloat16 [16, 2048, 512], P('grp'), may hold values from -5 to 5
- prefix_rope: bfloat16 [16, 64, 2048], P('grp'), may hold values from -8 to 8
- suffix_latent: bfloat16 [512, 256, 512], P(('grp', 'tp')), may hold values from -5 to 5
- suffix_rope: bfloat16 [512, 64, 256], P(('grp', 'tp')), may hold values from -4 to 4
- suffix_len: int32 [8, 64], P('grp'), may hold values from 1 to 256, 8192 in all within a row
- request_prefix: int32 [512], P('grp'), may hold values from 0 to 15, as said below
- prefix_slot: int32 [16], replicated, may hold values from 0 to 15, as said below
Outputs:
- attended: bfloat16 [512, 16384], P('grp', 'tp')
The draws below stay inside these ranges and needn't reach their ends.
Inputs may be any that keep to these rules, and one draw needn't show every extreme that they name: `request_prefix`: of the requests of one group, at most 8 name the same prefix; in every draw one prefix is named by exactly 8 requests of every group. `prefix_slot`: A permutation: each cache row holds exactly one prefix. `suffix_len`: the lengths of one group sum to 8192, and one of them is 256.
All inputs are finite; a program needn't handle non-finite values.
Results may differ from the reference program's by a relative error of at most 0.018.
Values may be sent and summed in bfloat16 or wider, within the bound.
A program may use at most 128 MiB of HBM per device.

```python
import math
import jax
import jax.numpy as jnp
import numpy as np
from jax import lax

HEADS = 128
LATENT = 512
ROPE_DIM = 64
NOPE_DIM = 128
VALUE_DIM = 128
REQ_DEV = 64
PLEN = 2048
SLEN = 256
GROUPS = 8
PREFIXES = 16
CAPP = 8
REQUESTS = 512


def route_draw(key):
    base_key = jax.random.fold_in(key, 101)
    hot_slot = jax.random.randint(jax.random.fold_in(base_key, 1), (), 0, PREFIXES)
    scores = jax.random.randint(jax.random.fold_in(base_key, 2), (GROUPS, PREFIXES * CAPP), 0, 1073741824)
    position = jnp.arange(PREFIXES * CAPP, dtype=jnp.int32)
    scores = jnp.where((position // CAPP)[None, :] == hot_slot, -1, scores)
    ranked = jnp.argsort(scores, axis=1, stable=True)[:, :REQ_DEV]
    shuffle_keys = jax.random.randint(jax.random.fold_in(base_key, 3), (GROUPS, REQ_DEV), 0, 1073741824)
    shuffle = jnp.argsort(shuffle_keys, axis=1, stable=True)
    chosen = jnp.take_along_axis(ranked, shuffle, axis=1)
    slot_ids = (chosen // CAPP).reshape(-1).astype(jnp.int32)
    permuted = jax.random.permutation(jax.random.fold_in(base_key, 4), PREFIXES).astype(jnp.int32)
    inverse = jnp.argsort(permuted).astype(jnp.int32)
    return (inverse[slot_ids], permuted)


def rope_table(key):
    drawn = jnp.clip(jax.random.normal(jax.random.fold_in(key, 202), (PREFIXES, ROPE_DIM, PLEN), jnp.float32), -4.0, 4.0)
    return drawn


def draw_request_prefix(key, part):
    return route_draw(key)[0]


def draw_prefix_slot(key, part):
    return route_draw(key)[1]


def draw_prefix_rope(key, part):
    return rope_table(key).astype(jnp.bfloat16)


def draw_q_rope(key, part):
    drawn = jnp.clip(jax.random.normal(jax.random.fold_in(key, 303), (REQUESTS, HEADS * ROPE_DIM), jnp.float32), -4.0, 4.0)
    return drawn.astype(jnp.bfloat16)


def shard_levels(key, dims, cuts, low, high):
    factor_of = 1.0
    for dim, parts in cuts:
        heights = jax.random.uniform(jax.random.fold_in(jax.random.fold_in(key, 6), dim), (parts,), jnp.float32, low / len(cuts), high / len(cuts))
        factor_of = factor_of * jnp.repeat(jnp.exp(heights), dims[dim] // parts).reshape((-1,) + (1,) * (len(dims) - 1 - dim))
    return factor_of


def length_profile(number_of, total, limit, skew):
    weights = [(1 << 20) // math.isqrt(standing ** skew) + 1 for standing in range(2, number_of + 1)]
    surplus, counts = total - limit - (number_of - 1), [1] * (number_of - 1)
    while surplus > 0:
        candidates = [i for i in range(number_of - 1) if counts[i] < limit]
        whole, budget = sum([weights[i] for i in candidates]), surplus
        for i in candidates:
            addition = min(limit - counts[i], max(1, budget * weights[i] // whole), surplus)
            counts[i] = counts[i] + addition
            surplus = surplus - addition
    return np.array([limit] + counts)


def uneven(stream_key, amount, total, limit, slope):
    if amount == 2:
        one = jax.random.randint(stream_key, (), max(1, total - limit), min(limit, total - 1) + 1)
        return jnp.stack([one, total - one])
    sizes = jnp.asarray(length_profile(amount, total, limit, slope), jnp.int32)
    couples = (amount - 1) // 2
    donor, receiver = sizes[1:1 + 2 * couples:2], sizes[2:2 + 2 * couples:2]
    slack = jnp.minimum(donor - 1, limit - receiver)
    shifted = jax.random.randint(jax.random.fold_in(stream_key, 1), (couples,), 0, 1 << 20) % (slack + 1)
    sizes = sizes.at[1:1 + 2 * couples:2].set(donor - shifted).at[2:2 + 2 * couples:2].set(receiver + shifted)
    return sizes[jax.random.permutation(jax.random.fold_in(stream_key, 2), amount)]


def normal_values(key, extent, spread, bound, pieces=(), kind=jnp.bfloat16):
    values = jax.random.normal(key, extent, jnp.float32) * spread
    if len(pieces) > 0:
        values = shard_levels(key, extent, pieces, -0.22, 0.18) * values
    return jnp.clip(values, min=-bound, max=bound).astype(kind)


def setup_inputs(seed: int = 0) -> dict:
    seeds = jax.random.split(jax.random.key(seed), 12)
    q_nope = normal_values(seeds[0], (REQUESTS, HEADS * NOPE_DIM), 1.25, 6.0, ((0, 8), (1, 4)))
    q_rope = draw_q_rope(jax.random.fold_in(seeds[11], 71), 0)
    w_uk = normal_values(seeds[2], (HEADS, NOPE_DIM, LATENT), NOPE_DIM ** -0.5, 0.5, ((0, 4),))
    w_uv = normal_values(seeds[3], (HEADS, LATENT, VALUE_DIM), (LATENT // 16) ** -0.5, 1.0, ((0, 4),))
    prefix_latent = normal_values(seeds[4], (PREFIXES, PLEN, LATENT), 1.0, 5.0, ((0, 8),))
    prefix_rope = draw_prefix_rope(jax.random.fold_in(seeds[11], 71), 0)
    suffix_latent = normal_values(seeds[6], (REQUESTS, SLEN, LATENT), 1.0, 5.0, ((0, 32),))
    suffix_rope = normal_values(seeds[7], (REQUESTS, ROPE_DIM, SLEN), 1.0, 4.0, ((0, 32),))
    suffix_len = jax.vmap(lambda own: uneven(own, REQ_DEV, REQ_DEV * SLEN // 2, SLEN, 2))(jax.random.split(seeds[8], GROUPS)).reshape((GROUPS, REQ_DEV)).astype(jnp.int32)
    request_prefix = draw_request_prefix(jax.random.fold_in(seeds[11], 71), 0)
    prefix_slot = draw_prefix_slot(jax.random.fold_in(seeds[11], 71), 0)
    return {"q_nope": q_nope, "q_rope": q_rope, "w_uk": w_uk, "w_uv": w_uv, "prefix_latent": prefix_latent, "prefix_rope": prefix_rope, "suffix_latent": suffix_latent, "suffix_rope": suffix_rope, "suffix_len": suffix_len, "request_prefix": request_prefix, "prefix_slot": prefix_slot}


def partial_attention(latent_q, rope_q, latent_rows, rope_cols, live_mask, score_scale):
    scores = jnp.dot(latent_q, latent_rows.T, preferred_element_type=jnp.float32)
    scores = (scores + jnp.dot(rope_q, rope_cols, preferred_element_type=jnp.float32)) * score_scale
    scores = jnp.where(live_mask[None, :], scores, jnp.float32(-1e+30))
    highest = lax.optimization_barrier(jnp.max(scores, axis=1, keepdims=True))
    exponent = jnp.where(live_mask[None, :], jnp.exp(scores - highest), jnp.float32(0.0))
    summed = lax.optimization_barrier(jnp.sum(exponent, axis=1))
    weights = exponent.astype(jnp.bfloat16)
    latent_out = (jnp.dot(weights, latent_rows, preferred_element_type=jnp.float32) / summed[:, None]).astype(jnp.bfloat16)
    return (latent_out, highest[:, 0], summed)

def reference(q_nope, q_rope, w_uk, w_uv, prefix_latent, prefix_rope, suffix_latent, suffix_rope, suffix_len, request_prefix, prefix_slot):
    score_scale = 1.0 / math.sqrt(NOPE_DIM + ROPE_DIM)
    slot_ids = prefix_slot[request_prefix].astype(jnp.int32)
    lengths = suffix_len.reshape(-1).astype(jnp.int32)
    nope_heads = q_nope.reshape(REQUESTS, HEADS, NOPE_DIM).astype(jnp.float32)
    q_latent = jnp.einsum('rhd,hdc->rhc', nope_heads, w_uk.astype(jnp.float32)).astype(jnp.bfloat16)
    rope_heads = q_rope.reshape(REQUESTS, HEADS, ROPE_DIM)
    w_uv_wide = w_uv.astype(jnp.float32)
    positions = jnp.arange(SLEN, dtype=jnp.int32)
    prefix_live = jnp.ones((PLEN,), dtype=bool)

    def one_request(request_items):
        latent_q, rope_q, slot_id, suffix_rows, suffix_cols, length = request_items
        latent_rows = lax.dynamic_index_in_dim(prefix_latent, slot_id, 0, keepdims=False)
        rope_cols = lax.dynamic_index_in_dim(prefix_rope, slot_id, 0, keepdims=False)
        prefix_out, prefix_max, prefix_total = partial_attention(latent_q, rope_q, latent_rows, rope_cols, prefix_live, score_scale)
        prefix_values = jnp.einsum('hc,hcv->hv', prefix_out.astype(jnp.float32), w_uv_wide).astype(jnp.bfloat16)
        suffix_live = positions < length
        suffix_out, suffix_max, suffix_total = partial_attention(latent_q, rope_q, suffix_rows, suffix_cols, suffix_live, score_scale)
        suffix_values = jnp.einsum('hc,hcv->hv', suffix_out.astype(jnp.float32), w_uv_wide).astype(jnp.bfloat16)
        overall = jnp.maximum(prefix_max, suffix_max)
        prefix_share = prefix_total * jnp.exp(prefix_max - overall)
        suffix_share = suffix_total * jnp.exp(suffix_max - overall)
        mixed = prefix_share[:, None] * prefix_values.astype(jnp.float32) + suffix_share[:, None] * suffix_values.astype(jnp.float32)
        mixed = mixed / (prefix_share + suffix_share)[:, None]
        return mixed.astype(jnp.bfloat16).reshape(-1)
    return lax.map(one_request, (q_latent, rope_heads, slot_ids, suffix_latent, suffix_rope, lengths))
```

```python
import functools
import math

import jax
import jax.numpy as jnp
from jax import lax
from jax.experimental import pallas as pl
from jax.experimental.pallas import tpu as pltpu
from jax.sharding import PartitionSpec as P

MESH = pl.DeviceIdType.MESH
CHUNKS = 4
SPLIT = 2
F32 = jnp.float32
BF16 = jnp.bfloat16


def mm(a, b):
    return jnp.dot(a, b, preferred_element_type=F32)


def mm_t(a, b):
    return lax.dot_general(a, b, (((1,), (1,)), ((), ())), preferred_element_type=F32)


def kernel(dims, *refs):
    n, t, chunks, cap, score_scale = dims
    (q_nope, q_rope, placing, sending, perm, perm_t, sel, sel_t, lens) = refs[:9]
    hbm = refs[9:15]
    out = refs[15]
    held = refs[16:22]
    wuk, wuv, plat, prope, slat, srope = held
    (qs, qr, qh, tqs, tqr, tropes, rq, sos, sor, ssts, sstr, vbs, vbr, st, sts, strv, vall, svals) = refs[22:40]
    (load_sem, rope_ss, rope_rs, tq_ss, tq_rs, so_ss, so_rs, sst_ss, sst_rs, q_ss, q_rs, vb_ss, vb_rs, st_ss, st_rs) = refs[40:]
    g = lax.axis_index("grp")
    y = lax.axis_index("tp")
    batch = q_nope.shape[0]
    heads, nope, latent = wuk.shape
    rope = q_rope.shape[1] // heads
    value = wuv.shape[2]
    share = batch // t
    hc = heads // chunks
    nw, rw, vw = hc * nope, hc * rope, hc * value
    rows_in = sending.shape[0]
    pr = rows_in // n
    prefixes = plat.shape[0]
    per = n * cap

    def peer_g(d):
        return lax.rem(g + d, n)

    def peer_t(d):
        return lax.rem(y + d, t)

    loads = [pltpu.make_async_copy(a, b, load_sem.at[i]) for i, (a, b) in enumerate(zip(hbm, held))]
    for i in (0, 4, 5, 2, 3, 1):
        loads[i].start()

    barrier = pltpu.get_barrier_semaphore()

    def greet_g(d, _):
        pl.semaphore_signal(barrier, inc=1, device_id=(peer_g(d), y), device_id_type=MESH)
        return 0

    def greet_t(d, _):
        pl.semaphore_signal(barrier, inc=1, device_id=(g, peer_t(d)), device_id_type=MESH)
        return 0

    lax.fori_loop(1, n, greet_g, 0)
    lax.fori_loop(1, t, greet_t, 0)
    pl.semaphore_wait(barrier, n + t - 2)

    def rope_copy(to, at, sem):
        return pltpu.make_async_remote_copy(
            src_ref=q_rope.at[pl.ds(pl.multiple_of(to * share, share), share)],
            dst_ref=tropes.at[at],
            send_sem=rope_ss.at[sem],
            recv_sem=rope_rs.at[at],
            device_id=(g, to),
            device_id_type=MESH,
        )

    def t_copy(src, dst, ss, rs, to, at):
        return pltpu.make_async_remote_copy(
            src_ref=src, dst_ref=dst.at[at], send_sem=ss.at[to], recv_sem=rs.at[at],
            device_id=(g, to), device_id_type=MESH,
        )

    def g_copy(src, dst, ss, rs, to):
        return pltpu.make_async_remote_copy(
            src_ref=src, dst_ref=dst, send_sem=ss, recv_sem=rs,
            device_id=(to, y), device_id_type=MESH,
        )

    def each_t(fn):
        def body(d, _):
            fn(peer_t(d))
            return 0
        lax.fori_loop(1, t, body, 0)

    def each_g(fn):
        def body(d, _):
            fn(peer_g(d))
            return 0
        lax.fori_loop(1, n, body, 0)

    def q_copy(c, to, at):
        return g_copy(qs.at[c, to], qr.at[c, at], q_ss.at[c, to], q_rs.at[c, at], to)

    def v_copy(c, to, at):
        return g_copy(vbs.at[c, to], vbr.at[c, at], vb_ss.at[c, to], vb_rs.at[c, at], to)

    def s_copy(to, at):
        return g_copy(sts.at[to], strv.at[at], st_ss.at[to], st_rs.at[at], to)

    each_t(lambda to: rope_copy(to, y, to).start())

    for c in range(chunks):
        got = mm(sending[...], q_nope[:, c * nw:(c + 1) * nw]).astype(BF16)
        qs[c, :, :, :nw] = got.reshape(n, pr, nw)
        got = mm(sending[...], q_rope[:, c * rw:(c + 1) * rw]).astype(BF16)
        qs[c, :, :, nw:] = got.reshape(n, pr, rw)
        each_g(lambda to: q_copy(c, to, g).start())
        qr[c, g] = qs[c, g]

    tropes[y] = q_rope[pl.ds(pl.multiple_of(y * share, share), share), :]

    loads[0].wait()

    def own_latent(h, _):
        x = q_nope[:, pl.ds(pl.multiple_of(h * nope, nope), nope)]
        got = mm(x, wuk[h]).astype(BF16)
        qh[:, pl.ds(pl.multiple_of(h * share, share), share), :] = got.reshape(t, share, latent)
        return 0

    lax.fori_loop(0, heads, own_latent, 0, unroll=4)

    def send_latent(d, _):
        to = peer_t(d)
        tqs[to] = mm(perm[...], qh[to]).astype(BF16)
        t_copy(tqs.at[to], tqr, tq_ss, tq_rs, to, y).start()
        return 0

    lax.fori_loop(1, t, send_latent, 0)
    tqr[y] = mm(perm[...], qh[y]).astype(BF16)

    each_t(lambda at: rope_copy(at, at, at).wait_recv())

    def split_rope(s, _):
        x = tropes[s]
        stacked = jnp.concatenate([x[:, h * rope:(h + 1) * rope] for h in range(heads)], axis=0)
        rq[s] = mm(perm[...], stacked).astype(BF16)
        return 0

    lax.fori_loop(0, t, split_rope, 0)

    loads[4].wait()
    loads[5].wait()
    each_t(lambda at: t_copy(tqs.at[at], tqr, tq_ss, tq_rs, at, at).wait_recv())

    all_heads = heads * t
    slen = slat.shape[1]
    lane = lax.broadcasted_iota(jnp.int32, (all_heads, 128), 1)

    def suffix_one(r, acc):
        rows = pl.ds(pl.multiple_of(r * heads, heads), heads)
        q = tqr[:, rows, :].reshape(all_heads, latent)
        qrope = rq[:, rows, :].reshape(all_heads, rope)
        s = mm_t(q, slat[r]) + mm(qrope, srope[r])
        length = lens[y * share + r]
        live = lax.broadcasted_iota(jnp.int32, (all_heads, slen), 1) < length
        s = jnp.where(live, s, F32(-1e30))
        high = jnp.max(s, axis=1, keepdims=True)
        e = jnp.where(live, jnp.exp((s - high) * score_scale), F32(0.0))
        total = jnp.sum(e, axis=1, keepdims=True)
        o = (mm(e.astype(BF16), slat[r]) / total).astype(BF16)
        sos[:, rows, :] = o.reshape(t, heads, latent)
        acc = jnp.where(lane == r, high * score_scale, acc)
        return jnp.where(lane == share + r, total, acc)

    acc = lax.fori_loop(0, share, suffix_one, jnp.zeros((all_heads, 128), F32), unroll=4)
    ssts[...] = jnp.transpose(acc)[:2 * share, :]

    def send_suffix(to):
        t_copy(sos.at[to], sor, so_ss, so_rs, to, y).start()
        t_copy(ssts, sstr, sst_ss, sst_rs, to, y).start()

    each_t(send_suffix)
    sor[y] = sos[y]
    sstr[y] = ssts[...]

    loads[2].wait()
    loads[3].wait()
    loads[1].wait()

    st[...] = jnp.zeros_like(st)
    stat_lane = lax.broadcasted_iota(jnp.int32, (per, 128), 1)
    ht = hc // SPLIT

    def chunk(c, _):
        each_g(lambda at: q_copy(c, at, at).wait_recv())
        x = mm(sel[...], qr[c].reshape(rows_in, nw + rw)).astype(BF16)
        for p in range(prefixes):
            mine = x[p * per:(p + 1) * per]
            stats = st[p * per:(p + 1) * per, :]
            for part in range(SPLIT):
                hs = range(part * ht, (part + 1) * ht)
                q = jnp.concatenate(
                    [mm(mine[:, i * nope:(i + 1) * nope], wuk[c * hc + i]).astype(BF16) for i in hs], axis=0)
                qp = jnp.concatenate(
                    [mine[:, nw + i * rope:nw + (i + 1) * rope] for i in hs], axis=0)
                s = mm_t(q, plat[p]) + mm(qp, prope[p])
                high = jnp.max(s, axis=1, keepdims=True)
                e = jnp.exp((s - high) * score_scale)
                total = jnp.sum(e, axis=1, keepdims=True)
                o = (mm(e.astype(BF16), plat[p]) / total).astype(BF16)
                for k, i in enumerate(hs):
                    h = c * hc + i
                    block = slice(k * per, (k + 1) * per)
                    vall[p * per:(p + 1) * per, i * value:(i + 1) * value] = mm(o[block], wuv[h]).astype(BF16)
                    stats = jnp.where(stat_lane == h, high[block] * score_scale, stats)
                    stats = jnp.where(stat_lane == 64 + h, total[block], stats)
            st[p * per:(p + 1) * per, :] = stats
        vbs[c] = mm(sel_t[...], vall[...]).astype(BF16).reshape(n, pr, vw)
        each_g(lambda to: v_copy(c, to, g).start())
        vbr[c, g] = vbs[c, g]
        return 0

    lax.fori_loop(0, chunks, chunk, 0)
    sts[...] = jnp.dot(
        sel_t[...].astype(F32), st[...], precision=lax.Precision.HIGHEST, preferred_element_type=F32
    ).reshape(n, pr, 128)
    each_g(lambda to: s_copy(to, g).start())
    strv[g] = sts[g]

    def wait_suffix(at):
        t_copy(sos.at[at], sor, so_ss, so_rs, at, at).wait_recv()
        t_copy(ssts, sstr, sst_ss, sst_rs, at, at).wait_recv()

    each_t(wait_suffix)

    def unsort(s, _):
        qh[s] = mm(perm_t[...], sor[s]).astype(BF16)
        return 0

    lax.fori_loop(0, t, unsort, 0)

    def own_values(h, _):
        o = qh[:, pl.ds(pl.multiple_of(h * share, share), share), :].reshape(batch, latent)
        svals[:, pl.ds(pl.multiple_of(h * value, value), value)] = mm(o, wuv[h]).astype(BF16)
        return 0

    lax.fori_loop(0, heads, own_values, 0, unroll=4)

    each_g(lambda at: s_copy(at, at).wait_recv())
    pst = jnp.dot(
        placing[...].astype(F32), strv[...].reshape(rows_in, 128),
        precision=lax.Precision.HIGHEST, preferred_element_type=F32)
    pmax, ptotal = pst[:, :heads], pst[:, 64:64 + heads]
    sst = sstr[...]
    shift = lax.rem(128 - y * heads, 128)
    smax = pltpu.roll(sst[:, :share, :].reshape(batch, 128), shift, 1)[:, :heads]
    stotal = pltpu.roll(sst[:, share:, :].reshape(batch, 128), shift, 1)[:, :heads]
    overall = jnp.maximum(pmax, smax)
    pshare = ptotal * jnp.exp(pmax - overall)
    sshare = stotal * jnp.exp(smax - overall)
    both = pshare + sshare
    pshare = pshare / both
    sshare = sshare / both

    for c in range(chunks):
        each_g(lambda at: v_copy(c, at, at).wait_recv())
        pv = mm(placing[...], vbr[c].reshape(rows_in, vw))
        for i in range(hc):
            h = c * hc + i
            sv = svals[:, h * value:(h + 1) * value].astype(F32)
            mixed = pshare[:, h:h + 1] * pv[:, i * value:(i + 1) * value] + sshare[:, h:h + 1] * sv
            out[:, h * value:(h + 1) * value] = mixed.astype(BF16)

    each_t(lambda to: rope_copy(to, y, to).wait_send())
    each_t(lambda to: t_copy(tqs.at[to], tqr, tq_ss, tq_rs, to, y).wait_send())
    each_t(lambda to: t_copy(sos.at[to], sor, so_ss, so_rs, to, y).wait_send())
    each_t(lambda to: t_copy(ssts, sstr, sst_ss, sst_rs, to, y).wait_send())
    each_g(lambda to: s_copy(to, g).wait_send())

    def drain(c, _):
        each_g(lambda to: q_copy(c, to, g).wait_send())
        each_g(lambda to: v_copy(c, to, g).wait_send())
        return 0

    lax.fori_loop(0, chunks, drain, 0)


def local(
    q_nope, q_rope, w_uk, w_uv, prefix_latent, prefix_rope,
    suffix_latent, suffix_rope, suffix_len, request_prefix, prefix_slot,
):
    n = lax.axis_size("grp")
    t = lax.axis_size("tp")
    batch = q_nope.shape[0]
    heads, nope, latent = w_uk.shape
    value = w_uv.shape[2]
    rope = q_rope.shape[1] // heads
    prefixes = prefix_slot.shape[0]
    own = prefix_latent.shape[0]
    cap = max(2, 2 * batch // prefixes)
    pr = -(-own * cap // 16) * 16
    share = batch // t
    chunks = CHUNKS
    score_scale = 1.0 / math.sqrt(nope + rope)

    ids = jnp.arange(prefixes, dtype=jnp.int32)
    naming = (request_prefix[:, None] == ids[None, :]).astype(jnp.int32)
    slot_ids = jnp.sum(naming * prefix_slot[None, :], axis=1)
    hits = (slot_ids[:, None] == ids[None, :]).astype(jnp.int32)
    earlier = jnp.cumsum(hits, axis=0) - hits
    base = (ids // own) * pr + (ids % own) * cap
    dest = jnp.sum((earlier + base[None, :]) * hits, axis=1)
    rows = jnp.arange(n * pr, dtype=jnp.int32)
    placing = (dest[:, None] == rows[None, :]).astype(BF16)
    sending = (rows[:, None] == dest[None, :]).astype(BF16)

    i = jnp.arange(heads * share, dtype=jnp.int32)
    target = (i % heads) * share + i // heads
    perm = (target[:, None] == i[None, :]).astype(BF16)
    perm_t = (i[:, None] == target[None, :]).astype(BF16)
    k = jnp.arange(own * n * cap, dtype=jnp.int32)
    where = ((k // cap) % n) * pr + (k // (n * cap)) * cap + k % cap
    sel = (where[:, None] == rows[None, :]).astype(BF16)
    sel_t = (rows[:, None] == where[None, :]).astype(BF16)

    hc = heads // chunks
    width = hc * (nope + rope)
    vm = pl.BlockSpec(memory_space=pltpu.VMEM)
    anyspec = pl.BlockSpec(memory_space=pl.ANY)
    big = (w_uk, w_uv, prefix_latent, prefix_rope, suffix_latent, suffix_rope)
    V = pltpu.VMEM
    D = pltpu.SemaphoreType.DMA
    scratch = [V(a.shape, a.dtype) for a in big] + [
        V((chunks, n, pr, width), BF16),
        V((chunks, n, pr, width), BF16),
        V((t, heads * share, latent), BF16),
        V((t, heads * share, latent), BF16),
        V((t, heads * share, latent), BF16),
        V((t, share, heads * rope), BF16),
        V((t, heads * share, rope), BF16),
        V((t, heads * share, latent), BF16),
        V((t, heads * share, latent), BF16),
        V((2 * share, 128), F32),
        V((t, 2 * share, 128), F32),
        V((chunks, n, pr, hc * value), BF16),
        V((chunks, n, pr, hc * value), BF16),
        V((own * n * cap, 128), F32),
        V((n, pr, 128), F32),
        V((n, pr, 128), F32),
        V((own * n * cap, hc * value), BF16),
        V((batch, heads * value), BF16),
        D((6,)), D((t,)), D((t,)), D((t,)), D((t,)), D((t,)), D((t,)), D((t,)), D((t,)),
        D((chunks, n)), D((chunks, n)), D((chunks, n)), D((chunks, n)), D((n,)), D((n,)),
    ]
    return pl.pallas_call(
        functools.partial(kernel, (n, t, chunks, cap, score_scale)),
        out_shape=jax.ShapeDtypeStruct((batch, heads * value), BF16),
        in_specs=[vm] * 8 + [pl.BlockSpec(memory_space=pltpu.SMEM)] + [anyspec] * 6,
        out_specs=vm,
        scratch_shapes=scratch,
        compiler_params=pltpu.CompilerParams(
            collective_id=0, has_side_effects=True, vmem_limit_bytes=63 * 1024 * 1024),
    )(q_nope, q_rope, placing, sending, perm, perm_t, sel, sel_t, suffix_len.reshape(-1), *big)


def solution(mesh):
    in_specs = (
        P("grp", "tp"),
        P("grp", "tp"),
        P("tp", None, None),
        P("tp", None, None),
        P("grp", None, None),
        P("grp", None, None),
        P(("grp", "tp"), None, None),
        P(("grp", "tp"), None, None),
        P("grp", None),
        P("grp"),
        P(),
    )
    return jax.shard_map(local, mesh=mesh, in_specs=in_specs, out_specs=P("grp", "tp"), check_vma=False)
```

```python
import functools
import math

import jax
import jax.numpy as jnp
from jax import lax
from jax.experimental import pallas as pl
from jax.experimental.pallas import tpu as pltpu
from jax.sharding import PartitionSpec as P

MESH = pl.DeviceIdType.MESH
CHUNKS = 4
SPLIT = 2
F32 = jnp.float32
BF16 = jnp.bfloat16


HALVES = 2


def quotient(x, k):
    return x >> (k.bit_length() - 1) if k & (k - 1) == 0 else x // k


def remainder(x, k):
    return x & (k - 1) if k & (k - 1) == 0 else x % k


def iotas(rows, columns):
    shape = (rows, columns)
    return lax.broadcasted_iota(jnp.int32, shape, 0), lax.broadcasted_iota(jnp.int32, shape, 1)


def one_hot(x):
    return x.astype(F32).astype(BF16)


def mm(a, b):
    return jnp.dot(a, b, preferred_element_type=F32)


def mm_t(a, b):
    return lax.dot_general(a, b, (((1,), (1,)), ((), ())), preferred_element_type=F32)


def kernel(dims, *refs):
    n, t, chunks, cap, score_scale = dims
    (q_nope, q_rope, named, slots, lens) = refs[:5]
    hbm = refs[5:11]
    out = refs[11]
    held = refs[12:18]
    wuk, wuv, plat, prope, slat, srope = held
    (qs, qr, qh, tqs, tqr, tropes, rq, sos, sor, ssts, sstr, vbs, vbr, st, sts, strv, vall, svals,
     sending, perm, perm_t, sel, sel_t, acc) = refs[18:42]
    (load_sem, rope_ss, rope_rs, tq_ss, tq_rs, so_ss, so_rs, sst_ss, sst_rs, q_ss, q_rs, vb_ss, vb_rs, st_ss, st_rs) = refs[42:]
    g = lax.axis_index("grp")
    y = lax.axis_index("tp")
    batch = q_nope.shape[0]
    heads, nope, latent = wuk.shape
    rope = q_rope.shape[1] // heads
    value = wuv.shape[2]
    share = batch // t
    hc = heads // chunks
    nw, rw, vw = hc * nope, hc * rope, hc * value
    pr = qs.shape[2]
    rows_in = n * pr
    prefixes = plat.shape[0]
    per = n * cap

    def peer_g(d):
        return lax.rem(g + d, n)

    def peer_t(d):
        return lax.rem(y + d, t)

    loads = [pltpu.make_async_copy(a, b, load_sem.at[i]) for i, (a, b) in enumerate(zip(hbm, held))]
    for i in (0, 4, 5, 2, 3, 1):
        loads[i].start()

    barrier = pltpu.get_barrier_semaphore()

    def greet_g(d, _):
        pl.semaphore_signal(barrier, inc=1, device_id=(peer_g(d), y), device_id_type=MESH)
        return 0

    def greet_t(d, _):
        pl.semaphore_signal(barrier, inc=1, device_id=(g, peer_t(d)), device_id_type=MESH)
        return 0

    lax.fori_loop(1, n, greet_g, 0)
    lax.fori_loop(1, t, greet_t, 0)
    pl.semaphore_wait(barrier, n + t - 2)

    def rope_copy(to, at, sem):
        return pltpu.make_async_remote_copy(
            src_ref=q_rope.at[pl.ds(pl.multiple_of(to * share, share), share)],
            dst_ref=tropes.at[at],
            send_sem=rope_ss.at[sem],
            recv_sem=rope_rs.at[at],
            device_id=(g, to),
            device_id_type=MESH,
        )

    def t_copy(src, dst, ss, rs, to, at):
        return pltpu.make_async_remote_copy(
            src_ref=src, dst_ref=dst.at[at], send_sem=ss.at[to], recv_sem=rs.at[at],
            device_id=(g, to), device_id_type=MESH,
        )

    half = heads * share // HALVES

    def tq_copy(a, to, at):
        rows = pl.ds(pl.multiple_of(a * half, half), half)
        return pltpu.make_async_remote_copy(
            src_ref=tqs.at[to, rows], dst_ref=tqr.at[at, rows],
            send_sem=tq_ss.at[a, to], recv_sem=tq_rs.at[a, at],
            device_id=(g, to), device_id_type=MESH,
        )

    def so_copy(a, to, at):
        rows = pl.ds(pl.multiple_of(a * half, half), half)
        return pltpu.make_async_remote_copy(
            src_ref=sos.at[to, rows], dst_ref=sor.at[at, rows],
            send_sem=so_ss.at[a, to], recv_sem=so_rs.at[a, at],
            device_id=(g, to), device_id_type=MESH,
        )

    def g_copy(src, dst, ss, rs, to):
        return pltpu.make_async_remote_copy(
            src_ref=src, dst_ref=dst, send_sem=ss, recv_sem=rs,
            device_id=(to, y), device_id_type=MESH,
        )

    def each_t(fn):
        def body(d, _):
            fn(peer_t(d))
            return 0
        lax.fori_loop(1, t, body, 0)

    def each_g(fn):
        def body(d, _):
            fn(peer_g(d))
            return 0
        lax.fori_loop(1, n, body, 0)

    def q_copy(c, to, at):
        return g_copy(qs.at[c, to], qr.at[c, at], q_ss.at[c, to], q_rs.at[c, at], to)

    def v_copy(c, to, at):
        return g_copy(vbs.at[c, to], vbr.at[c, at], vb_ss.at[c, to], vb_rs.at[c, at], to)

    def s_copy(to, at):
        return g_copy(sts.at[to], strv.at[at], st_ss.at[to], st_rs.at[at], to)

    each_t(lambda to: rope_copy(to, y, to).start())

    who = named[...]
    slot = jnp.zeros_like(who)
    for k in range(n * prefixes):
        slot = jnp.where(who == k, slots[0, k], slot)
    row, _ = iotas(n * prefixes, batch)
    hits = (row == slot).astype(F32)
    first, second = iotas(batch, batch)
    earlier = mm(hits.astype(BF16), one_hot(first < second))
    base = quotient(row, prefixes) * pr + remainder(row, prefixes) * cap
    dest = jnp.sum(hits * (earlier + base.astype(F32)), axis=0, keepdims=True).astype(jnp.int32)
    row, _ = iotas(rows_in, batch)
    sending[...] = (row == dest).astype(F32)
    send_hot = sending[...].astype(BF16)

    for c in range(chunks):
        got = mm(send_hot, q_nope[:, c * nw:(c + 1) * nw]).astype(BF16)
        qs[c, :, :, :nw] = got.reshape(n, pr, nw)
        got = mm(send_hot, q_rope[:, c * rw:(c + 1) * rw]).astype(BF16)
        qs[c, :, :, nw:] = got.reshape(n, pr, rw)
        each_g(lambda to: q_copy(c, to, g).start())
        qr[c, g] = qs[c, g]

    i, j = iotas(heads * share, heads * share)
    perm[...] = one_hot(j == remainder(i, heads) * share + quotient(i, heads))
    perm_t[...] = one_hot(i == remainder(j, heads) * share + quotient(j, heads))

    def place(k):
        return remainder(quotient(k, cap), n) * pr + quotient(k, n * cap) * cap + remainder(k, cap)

    i, j = iotas(prefixes * per, rows_in)
    sel[...] = one_hot(place(i) == j)
    i, j = iotas(rows_in, prefixes * per)
    sel_t[...] = one_hot(place(j) == i)

    tropes[y] = q_rope[pl.ds(pl.multiple_of(y * share, share), share), :]

    loads[0].wait()

    def own_latent(h, _):
        x = q_nope[:, pl.ds(pl.multiple_of(h * nope, nope), nope)]
        got = mm(x, wuk[h]).astype(BF16)
        qh[:, pl.ds(pl.multiple_of(h * share, share), share), :] = got.reshape(t, share, latent)
        return 0

    lax.fori_loop(0, heads, own_latent, 0, unroll=4)

    for a in range(HALVES):
        def send_latent(to):
            tqs[to, a * half:(a + 1) * half] = mm(perm[a * half:(a + 1) * half, :], qh[to]).astype(BF16)
            tq_copy(a, to, y).start()

        each_t(send_latent)
    tqr[y] = mm(perm[...], qh[y]).astype(BF16)

    all_heads = heads * t
    slen = slat.shape[1]
    lane = lax.broadcasted_iota(jnp.int32, (all_heads, 128), 1)

    def split_rope(s, _):
        x = tropes[s]
        stacked = jnp.concatenate([x[:, h * rope:(h + 1) * rope] for h in range(heads)], axis=0)
        rq[s] = mm(perm[...], stacked).astype(BF16)
        return 0

    def suffix_one(r, _):
        rows = pl.ds(pl.multiple_of(r * heads, heads), heads)
        q = tqr[:, rows, :].reshape(all_heads, latent)
        qrope = rq[:, rows, :].reshape(all_heads, rope)
        s = mm_t(q, slat[r]) + mm(qrope, srope[r])
        length = lens[0, y * share + r]
        live = lax.broadcasted_iota(jnp.int32, (all_heads, slen), 1) < length
        s = jnp.where(live, s, F32(-1e30))
        high = jnp.max(s, axis=1, keepdims=True)
        e = jnp.where(live, jnp.exp((s - high) * score_scale), F32(0.0))
        total = jnp.sum(e, axis=1, keepdims=True)
        o = (mm(e.astype(BF16), slat[r]) / total).astype(BF16)
        sos[:, rows, :] = o.reshape(t, heads, latent)
        stats = jnp.where(lane == r, high * score_scale, acc[...])
        acc[...] = jnp.where(lane == share + r, total, stats)
        return 0

    def suffix_half(a):
        @pl.when(a == 0)
        def _():
            each_t(lambda at: rope_copy(at, at, at).wait_recv())
            lax.fori_loop(0, t, split_rope, 0)
            loads[4].wait()
            loads[5].wait()
            acc[...] = jnp.zeros_like(acc)

        each_t(lambda at: tq_copy(a, at, at).wait_recv())
        some = share // HALVES

        def two(k, _):
            for u in range(2):
                suffix_one(a * some + k * 2 + u, 0)
            return 0

        lax.fori_loop(0, some // 2, two, 0)
        each_t(lambda to: so_copy(a, to, y).start())

        @pl.when(a == HALVES - 1)
        def _():
            ssts[...] = jnp.transpose(acc[...])[:2 * share, :]
            each_t(lambda to: t_copy(ssts, sstr, sst_ss, sst_rs, to, y).start())
            sor[y] = sos[y]
            sstr[y] = ssts[...]

    loads[2].wait()
    loads[3].wait()
    loads[1].wait()

    st[...] = jnp.zeros_like(st)
    stat_lane = lax.broadcasted_iota(jnp.int32, (per, 128), 1)
    ht = hc // SPLIT

    def chunk(c, _):
        each_g(lambda at: q_copy(c, at, at).wait_recv())
        x = mm(sel[...], qr[c].reshape(rows_in, nw + rw)).astype(BF16)
        for p in range(prefixes):
            mine = x[p * per:(p + 1) * per]
            stats = st[p * per:(p + 1) * per, :]
            for part in range(SPLIT):
                hs = range(part * ht, (part + 1) * ht)
                q = jnp.concatenate(
                    [mm(mine[:, i * nope:(i + 1) * nope], wuk[c * hc + i]).astype(BF16) for i in hs], axis=0)
                qp = jnp.concatenate(
                    [mine[:, nw + i * rope:nw + (i + 1) * rope] for i in hs], axis=0)
                s = mm_t(q, plat[p]) + mm(qp, prope[p])
                high = jnp.max(s, axis=1, keepdims=True)
                e = jnp.exp((s - high) * score_scale)
                total = jnp.sum(e, axis=1, keepdims=True)
                o = (mm(e.astype(BF16), plat[p]) / total).astype(BF16)
                for k, i in enumerate(hs):
                    h = c * hc + i
                    block = slice(k * per, (k + 1) * per)
                    vall[p * per:(p + 1) * per, i * value:(i + 1) * value] = mm(o[block], wuv[h]).astype(BF16)
                    stats = jnp.where(stat_lane == h, high[block] * score_scale, stats)
                    stats = jnp.where(stat_lane == 64 + h, total[block], stats)
            st[p * per:(p + 1) * per, :] = stats
        @pl.when(c == chunks - 1)
        def _():
            sts[...] = jnp.dot(
                sel_t[...].astype(F32), st[...], precision=lax.Precision.HIGHEST, preferred_element_type=F32
            ).reshape(n, pr, 128)
            each_g(lambda to: s_copy(to, g).start())
            strv[g] = sts[g]

        vbs[c] = mm(sel_t[...], vall[...]).astype(BF16).reshape(n, pr, vw)
        each_g(lambda to: v_copy(c, to, g).start())
        vbr[c, g] = vbs[c, g]

        @pl.when(c < HALVES)
        def _():
            suffix_half(c)

        return 0

    lax.fori_loop(0, chunks, chunk, 0)
    def wait_suffix(at):
        for a in range(HALVES):
            so_copy(a, at, at).wait_recv()
        t_copy(ssts, sstr, sst_ss, sst_rs, at, at).wait_recv()

    each_t(wait_suffix)

    def unsort(s, _):
        qh[s] = mm(perm_t[...], sor[s]).astype(BF16)
        return 0

    lax.fori_loop(0, t, unsort, 0)

    def own_values(h, _):
        o = qh[:, pl.ds(pl.multiple_of(h * share, share), share), :].reshape(batch, latent)
        svals[:, pl.ds(pl.multiple_of(h * value, value), value)] = mm(o, wuv[h]).astype(BF16)
        return 0

    lax.fori_loop(0, heads, own_values, 0, unroll=4)

    each_g(lambda at: s_copy(at, at).wait_recv())
    placed = jnp.transpose(sending[...])
    placing = placed.astype(BF16)
    pst = jnp.dot(
        placed, strv[...].reshape(rows_in, 128),
        precision=lax.Precision.HIGHEST, preferred_element_type=F32)
    pmax, ptotal = pst[:, :heads], pst[:, 64:64 + heads]
    sst = sstr[...]
    shift = lax.rem(128 - y * heads, 128)
    smax = pltpu.roll(sst[:, :share, :].reshape(batch, 128), shift, 1)[:, :heads]
    stotal = pltpu.roll(sst[:, share:, :].reshape(batch, 128), shift, 1)[:, :heads]
    overall = jnp.maximum(pmax, smax)
    pshare = ptotal * jnp.exp(pmax - overall)
    sshare = stotal * jnp.exp(smax - overall)
    both = pshare + sshare
    pshare = pshare / both
    sshare = sshare / both

    for c in range(chunks):
        each_g(lambda at: v_copy(c, at, at).wait_recv())
        pv = mm(placing, vbr[c].reshape(rows_in, vw))
        for i in range(hc):
            h = c * hc + i
            sv = svals[:, h * value:(h + 1) * value].astype(F32)
            mixed = pshare[:, h:h + 1] * pv[:, i * value:(i + 1) * value] + sshare[:, h:h + 1] * sv
            out[:, h * value:(h + 1) * value] = mixed.astype(BF16)

    each_t(lambda to: rope_copy(to, y, to).wait_send())
    for a in range(HALVES):
        each_t(lambda to: tq_copy(a, to, y).wait_send())
        each_t(lambda to: so_copy(a, to, y).wait_send())
    each_t(lambda to: t_copy(ssts, sstr, sst_ss, sst_rs, to, y).wait_send())
    each_g(lambda to: s_copy(to, g).wait_send())

    def drain(c, _):
        each_g(lambda to: q_copy(c, to, g).wait_send())
        each_g(lambda to: v_copy(c, to, g).wait_send())
        return 0

    lax.fori_loop(0, chunks, drain, 0)


def local(
    q_nope, q_rope, w_uk, w_uv, prefix_latent, prefix_rope,
    suffix_latent, suffix_rope, suffix_len, request_prefix, prefix_slot,
):
    n = lax.axis_size("grp")
    t = lax.axis_size("tp")
    batch = q_nope.shape[0]
    heads, nope, latent = w_uk.shape
    value = w_uv.shape[2]
    rope = q_rope.shape[1] // heads
    prefixes = prefix_slot.shape[0]
    own = prefix_latent.shape[0]
    cap = max(2, 2 * batch // prefixes)
    pr = -(-own * cap // 16) * 16
    share = batch // t
    chunks = CHUNKS
    score_scale = 1.0 / math.sqrt(nope + rope)

    hc = heads // chunks
    width = hc * (nope + rope)
    vm = pl.BlockSpec(memory_space=pltpu.VMEM)
    anyspec = pl.BlockSpec(memory_space=pl.ANY)
    big = (w_uk, w_uv, prefix_latent, prefix_rope, suffix_latent, suffix_rope)
    V = pltpu.VMEM
    D = pltpu.SemaphoreType.DMA
    scratch = [V(a.shape, a.dtype) for a in big] + [
        V((chunks, n, pr, width), BF16),
        V((chunks, n, pr, width), BF16),
        V((t, heads * share, latent), BF16),
        V((t, heads * share, latent), BF16),
        V((t, heads * share, latent), BF16),
        V((t, share, heads * rope), BF16),
        V((t, heads * share, rope), BF16),
        V((t, heads * share, latent), BF16),
        V((t, heads * share, latent), BF16),
        V((2 * share, 128), F32),
        V((t, 2 * share, 128), F32),
        V((chunks, n, pr, hc * value), BF16),
        V((chunks, n, pr, hc * value), BF16),
        V((own * n * cap, 128), F32),
        V((n, pr, 128), F32),
        V((n, pr, 128), F32),
        V((own * n * cap, hc * value), BF16),
        V((batch, heads * value), BF16),
        V((n * pr, batch), F32),
        V((heads * share, heads * share), BF16),
        V((heads * share, heads * share), BF16),
        V((own * n * cap, n * pr), BF16),
        V((n * pr, own * n * cap), BF16),
        V((heads * t, 128), F32),
        D((6,)), D((t,)), D((t,)), D((HALVES, t)), D((HALVES, t)), D((HALVES, t)), D((HALVES, t)), D((t,)), D((t,)),
        D((chunks, n)), D((chunks, n)), D((chunks, n)), D((chunks, n)), D((n,)), D((n,)),
    ]
    return pl.pallas_call(
        functools.partial(kernel, (n, t, chunks, cap, score_scale)),
        out_shape=jax.ShapeDtypeStruct((batch, heads * value), BF16),
        in_specs=[vm] * 3 + [pl.BlockSpec(memory_space=pltpu.SMEM)] * 2 + [anyspec] * 6,
        out_specs=vm,
        scratch_shapes=scratch,
        compiler_params=pltpu.CompilerParams(
            collective_id=0, has_side_effects=True, vmem_limit_bytes=63 * 1024 * 1024),
    )(q_nope, q_rope, request_prefix.reshape(1, -1), prefix_slot.reshape(1, -1), suffix_len, *big)


def solution(mesh):
    in_specs = (
        P("grp", "tp"),
        P("grp", "tp"),
        P("tp", None, None),
        P("tp", None, None),
        P("grp", None, None),
        P("grp", None, None),
        P(("grp", "tp"), None, None),
        P(("grp", "tp"), None, None),
        P("grp", None),
        P("grp"),
        P(),
    )
    return jax.shard_map(local, mesh=mesh, in_specs=in_specs, out_specs=P("grp", "tp"), check_vma=False)
```

```python
import functools
import math

import jax
import jax.numpy as jnp
from jax import lax
from jax.experimental import pallas as pl
from jax.experimental.pallas import tpu as pltpu
from jax.sharding import PartitionSpec as P

MESH = pl.DeviceIdType.MESH
CHUNKS = 8
SPLIT = 1
F32 = jnp.float32
BF16 = jnp.bfloat16


HALVES = 2
SUFFIX_AT = (2, 4)


def quotient(x, k):
    return x >> (k.bit_length() - 1) if k & (k - 1) == 0 else x // k


def remainder(x, k):
    return x & (k - 1) if k & (k - 1) == 0 else x % k


def iotas(rows, columns):
    shape = (rows, columns)
    return lax.broadcasted_iota(jnp.int32, shape, 0), lax.broadcasted_iota(jnp.int32, shape, 1)


def one_hot(x):
    return x.astype(F32).astype(BF16)


def mm(a, b):
    return jnp.dot(a, b, preferred_element_type=F32)


def mm_t(a, b):
    return lax.dot_general(a, b, (((1,), (1,)), ((), ())), preferred_element_type=F32)


def kernel(dims, *refs):
    n, t, chunks, cap, score_scale = dims
    (q_nope, q_rope, named, slots, lens) = refs[:5]
    hbm = refs[5:11]
    out = refs[11]
    held = refs[12:18]
    wuk, wuv, plat, prope, slat, srope = held
    (qs, qr, qh, tqs, tqr, tropes, rq, sos, sor, ssts, sstr, vbs, vbr, st, sts, strv, vall, svals,
     sending, perm, perm_t, sel, sel_t, acc) = refs[18:42]
    (load_sem, rope_ss, rope_rs, tq_ss, tq_rs, so_ss, so_rs, sst_ss, sst_rs, q_ss, q_rs, vb_ss, vb_rs, st_ss, st_rs) = refs[42:]
    g = lax.axis_index("grp")
    y = lax.axis_index("tp")
    batch = q_nope.shape[0]
    heads, nope, latent = wuk.shape
    rope = q_rope.shape[1] // heads
    value = wuv.shape[2]
    share = batch // t
    hc = heads // chunks
    nw, rw, vw = hc * nope, hc * rope, hc * value
    pr = qs.shape[2]
    rows_in = n * pr
    prefixes = plat.shape[0]
    per = n * cap

    def peer_g(d):
        return lax.rem(g + d, n)

    def peer_t(d):
        return lax.rem(y + d, t)

    loads = [pltpu.make_async_copy(a, b, load_sem.at[i]) for i, (a, b) in enumerate(zip(hbm, held))]
    for i in (0, 4, 5, 2, 3, 1):
        loads[i].start()

    barrier = pltpu.get_barrier_semaphore()

    def greet_g(d, _):
        pl.semaphore_signal(barrier, inc=1, device_id=(peer_g(d), y), device_id_type=MESH)
        return 0

    def greet_t(d, _):
        pl.semaphore_signal(barrier, inc=1, device_id=(g, peer_t(d)), device_id_type=MESH)
        return 0

    lax.fori_loop(1, n, greet_g, 0)
    lax.fori_loop(1, t, greet_t, 0)
    pl.semaphore_wait(barrier, n + t - 2)

    def rope_copy(to, at, sem):
        return pltpu.make_async_remote_copy(
            src_ref=q_rope.at[pl.ds(pl.multiple_of(to * share, share), share)],
            dst_ref=tropes.at[at],
            send_sem=rope_ss.at[sem],
            recv_sem=rope_rs.at[at],
            device_id=(g, to),
            device_id_type=MESH,
        )

    def t_copy(src, dst, ss, rs, to, at):
        return pltpu.make_async_remote_copy(
            src_ref=src, dst_ref=dst.at[at], send_sem=ss.at[to], recv_sem=rs.at[at],
            device_id=(g, to), device_id_type=MESH,
        )

    half = heads * share // HALVES

    def tq_copy(a, to, at):
        rows = pl.ds(pl.multiple_of(a * half, half), half)
        return pltpu.make_async_remote_copy(
            src_ref=tqs.at[to, rows], dst_ref=tqr.at[at, rows],
            send_sem=tq_ss.at[a, to], recv_sem=tq_rs.at[a, at],
            device_id=(g, to), device_id_type=MESH,
        )

    def so_copy(a, to, at):
        rows = pl.ds(pl.multiple_of(a * half, half), half)
        return pltpu.make_async_remote_copy(
            src_ref=sos.at[to, rows], dst_ref=sor.at[at, rows],
            send_sem=so_ss.at[a, to], recv_sem=so_rs.at[a, at],
            device_id=(g, to), device_id_type=MESH,
        )

    def g_copy(src, dst, ss, rs, to):
        return pltpu.make_async_remote_copy(
            src_ref=src, dst_ref=dst, send_sem=ss, recv_sem=rs,
            device_id=(to, y), device_id_type=MESH,
        )

    def each_t(fn):
        def body(d, _):
            fn(peer_t(d))
            return 0
        lax.fori_loop(1, t, body, 0)

    def each_g(fn):
        def body(d, _):
            fn(peer_g(d))
            return 0
        lax.fori_loop(1, n, body, 0)

    def q_copy(c, to, at):
        return g_copy(qs.at[c, to], qr.at[c, at], q_ss.at[c, to], q_rs.at[c, at], to)

    def v_copy(c, to, at):
        return g_copy(vbs.at[c, to], vbr.at[c, at], vb_ss.at[c, to], vb_rs.at[c, at], to)

    def s_copy(to, at):
        return g_copy(sts.at[to], strv.at[at], st_ss.at[to], st_rs.at[at], to)

    each_t(lambda to: rope_copy(to, y, to).start())

    who = named[...]
    slot = jnp.zeros_like(who)
    for k in range(n * prefixes):
        slot = jnp.where(who == k, slots[0, k], slot)
    row, _ = iotas(n * prefixes, batch)
    hits = (row == slot).astype(F32)
    first, second = iotas(batch, batch)
    earlier = mm(hits.astype(BF16), one_hot(first < second))
    base = quotient(row, prefixes) * pr + remainder(row, prefixes) * cap
    dest = jnp.sum(hits * (earlier + base.astype(F32)), axis=0, keepdims=True).astype(jnp.int32)
    row, _ = iotas(rows_in, batch)
    sending[...] = (row == dest).astype(F32)
    send_hot = sending[...].astype(BF16)

    for c in range(chunks):
        got = mm(send_hot, q_nope[:, c * nw:(c + 1) * nw]).astype(BF16)
        qs[c, :, :, :nw] = got.reshape(n, pr, nw)
        got = mm(send_hot, q_rope[:, c * rw:(c + 1) * rw]).astype(BF16)
        qs[c, :, :, nw:] = got.reshape(n, pr, rw)
        each_g(lambda to: q_copy(c, to, g).start())
        qr[c, g] = qs[c, g]

    i, j = iotas(heads * share, heads * share)
    perm[...] = one_hot(j == remainder(i, heads) * share + quotient(i, heads))
    perm_t[...] = one_hot(i == remainder(j, heads) * share + quotient(j, heads))

    def place(k):
        return remainder(quotient(k, cap), n) * pr + quotient(k, n * cap) * cap + remainder(k, cap)

    i, j = iotas(prefixes * per, rows_in)
    sel[...] = one_hot(place(i) == j)
    i, j = iotas(rows_in, prefixes * per)
    sel_t[...] = one_hot(place(j) == i)

    tropes[y] = q_rope[pl.ds(pl.multiple_of(y * share, share), share), :]

    loads[0].wait()

    def own_latent(h, _):
        x = q_nope[:, pl.ds(pl.multiple_of(h * nope, nope), nope)]
        got = mm(x, wuk[h]).astype(BF16)
        qh[:, pl.ds(pl.multiple_of(h * share, share), share), :] = got.reshape(t, share, latent)
        return 0

    lax.fori_loop(0, heads, own_latent, 0, unroll=4)

    for a in range(HALVES):
        def send_latent(to):
            tqs[to, a * half:(a + 1) * half] = mm(perm[a * half:(a + 1) * half, :], qh[to]).astype(BF16)
            tq_copy(a, to, y).start()

        each_t(send_latent)
    tqr[y] = mm(perm[...], qh[y]).astype(BF16)

    all_heads = heads * t
    slen = slat.shape[1]
    lane = lax.broadcasted_iota(jnp.int32, (all_heads, 128), 1)

    def split_rope(s, _):
        x = tropes[s]
        stacked = jnp.concatenate([x[:, h * rope:(h + 1) * rope] for h in range(heads)], axis=0)
        rq[s] = mm(perm[...], stacked).astype(BF16)
        return 0

    def suffix_one(r, _):
        rows = pl.ds(pl.multiple_of(r * heads, heads), heads)
        q = tqr[:, rows, :].reshape(all_heads, latent)
        qrope = rq[:, rows, :].reshape(all_heads, rope)
        s = mm_t(q, slat[r]) + mm(qrope, srope[r])
        length = lens[0, y * share + r]
        live = lax.broadcasted_iota(jnp.int32, (all_heads, slen), 1) < length
        s = jnp.where(live, s, F32(-1e30))
        high = jnp.max(s, axis=1, keepdims=True)
        e = jnp.where(live, jnp.exp((s - high) * score_scale), F32(0.0))
        total = jnp.sum(e, axis=1, keepdims=True)
        o = (mm(e.astype(BF16), slat[r]) / total).astype(BF16)
        sos[:, rows, :] = o.reshape(t, heads, latent)
        stats = jnp.where(lane == r, high * score_scale, acc[...])
        acc[...] = jnp.where(lane == share + r, total, stats)
        return 0

    def suffix_half(a):
        if a == 0:
            each_t(lambda at: rope_copy(at, at, at).wait_recv())
            lax.fori_loop(0, t, split_rope, 0)
            loads[4].wait()
            loads[5].wait()
            acc[...] = jnp.zeros_like(acc)

        each_t(lambda at: tq_copy(a, at, at).wait_recv())
        some = share // HALVES

        def two(k, _):
            for u in range(2):
                suffix_one(a * some + k * 2 + u, 0)
            return 0

        lax.fori_loop(0, some // 2, two, 0)
        each_t(lambda to: so_copy(a, to, y).start())

        if a == HALVES - 1:
            ssts[...] = jnp.transpose(acc[...])[:2 * share, :]
            each_t(lambda to: t_copy(ssts, sstr, sst_ss, sst_rs, to, y).start())
            sor[y] = sos[y]
            sstr[y] = ssts[...]

    loads[2].wait()
    loads[3].wait()
    loads[1].wait()

    st[...] = jnp.zeros_like(st)
    stat_lane = lax.broadcasted_iota(jnp.int32, (per, 128), 1)
    ht = hc // SPLIT

    def chunk(c, _):
        each_g(lambda at: q_copy(c, at, at).wait_recv())
        x = mm(sel[...], qr[c].reshape(rows_in, nw + rw)).astype(BF16)
        for p in range(prefixes):
            mine = x[p * per:(p + 1) * per]
            stats = st[p * per:(p + 1) * per, :]
            for part in range(SPLIT):
                hs = range(part * ht, (part + 1) * ht)
                q = jnp.concatenate(
                    [mm(mine[:, i * nope:(i + 1) * nope], wuk[c * hc + i]).astype(BF16) for i in hs], axis=0)
                qp = jnp.concatenate(
                    [mine[:, nw + i * rope:nw + (i + 1) * rope] for i in hs], axis=0)
                s = mm_t(q, plat[p]) + mm(qp, prope[p])
                high = jnp.max(s, axis=1, keepdims=True)
                e = jnp.exp((s - high) * score_scale)
                total = jnp.sum(e, axis=1, keepdims=True)
                o = (mm(e.astype(BF16), plat[p]) / total).astype(BF16)
                for k, i in enumerate(hs):
                    h = c * hc + i
                    block = slice(k * per, (k + 1) * per)
                    vall[p * per:(p + 1) * per, i * value:(i + 1) * value] = mm(o[block], wuv[h]).astype(BF16)
                    stats = jnp.where(stat_lane == h, high[block] * score_scale, stats)
                    stats = jnp.where(stat_lane == 64 + h, total[block], stats)
            st[p * per:(p + 1) * per, :] = stats
        @pl.when(c == chunks - 1)
        def _():
            sts[...] = jnp.dot(
                sel_t[...].astype(F32), st[...], precision=lax.Precision.HIGHEST, preferred_element_type=F32
            ).reshape(n, pr, 128)
            each_g(lambda to: s_copy(to, g).start())
            strv[g] = sts[g]

        vbs[c] = mm(sel_t[...], vall[...]).astype(BF16).reshape(n, pr, vw)
        each_g(lambda to: v_copy(c, to, g).start())
        vbr[c, g] = vbs[c, g]

        for a, at in enumerate(SUFFIX_AT):
            @pl.when(c == at)
            def _():
                suffix_half(a)

        return 0

    lax.fori_loop(0, chunks, chunk, 0)
    def wait_suffix(at):
        for a in range(HALVES):
            so_copy(a, at, at).wait_recv()
        t_copy(ssts, sstr, sst_ss, sst_rs, at, at).wait_recv()

    each_t(wait_suffix)

    def unsort(s, _):
        qh[s] = mm(perm_t[...], sor[s]).astype(BF16)
        return 0

    lax.fori_loop(0, t, unsort, 0)

    def own_values(h, _):
        o = qh[:, pl.ds(pl.multiple_of(h * share, share), share), :].reshape(batch, latent)
        svals[:, pl.ds(pl.multiple_of(h * value, value), value)] = mm(o, wuv[h]).astype(BF16)
        return 0

    lax.fori_loop(0, heads, own_values, 0, unroll=4)

    each_g(lambda at: s_copy(at, at).wait_recv())
    placed = jnp.transpose(sending[...])
    placing = placed.astype(BF16)
    pst = jnp.dot(
        placed, strv[...].reshape(rows_in, 128),
        precision=lax.Precision.HIGHEST, preferred_element_type=F32)
    pmax, ptotal = pst[:, :heads], pst[:, 64:64 + heads]
    sst = sstr[...]
    shift = lax.rem(128 - y * heads, 128)
    smax = pltpu.roll(sst[:, :share, :].reshape(batch, 128), shift, 1)[:, :heads]
    stotal = pltpu.roll(sst[:, share:, :].reshape(batch, 128), shift, 1)[:, :heads]
    overall = jnp.maximum(pmax, smax)
    pshare = ptotal * jnp.exp(pmax - overall)
    sshare = stotal * jnp.exp(smax - overall)
    both = pshare + sshare
    pshare = pshare / both
    sshare = sshare / both

    for c in range(chunks):
        each_g(lambda at: v_copy(c, at, at).wait_recv())
        pv = mm(placing, vbr[c].reshape(rows_in, vw))
        for i in range(hc):
            h = c * hc + i
            sv = svals[:, h * value:(h + 1) * value].astype(F32)
            mixed = pshare[:, h:h + 1] * pv[:, i * value:(i + 1) * value] + sshare[:, h:h + 1] * sv
            out[:, h * value:(h + 1) * value] = mixed.astype(BF16)

    each_t(lambda to: rope_copy(to, y, to).wait_send())
    for a in range(HALVES):
        each_t(lambda to: tq_copy(a, to, y).wait_send())
        each_t(lambda to: so_copy(a, to, y).wait_send())
    each_t(lambda to: t_copy(ssts, sstr, sst_ss, sst_rs, to, y).wait_send())
    each_g(lambda to: s_copy(to, g).wait_send())

    def drain(c, _):
        each_g(lambda to: q_copy(c, to, g).wait_send())
        each_g(lambda to: v_copy(c, to, g).wait_send())
        return 0

    lax.fori_loop(0, chunks, drain, 0)


def local(
    q_nope, q_rope, w_uk, w_uv, prefix_latent, prefix_rope,
    suffix_latent, suffix_rope, suffix_len, request_prefix, prefix_slot,
):
    n = lax.axis_size("grp")
    t = lax.axis_size("tp")
    batch = q_nope.shape[0]
    heads, nope, latent = w_uk.shape
    value = w_uv.shape[2]
    rope = q_rope.shape[1] // heads
    prefixes = prefix_slot.shape[0]
    own = prefix_latent.shape[0]
    cap = max(2, 2 * batch // prefixes)
    pr = -(-own * cap // 16) * 16
    share = batch // t
    chunks = CHUNKS
    score_scale = 1.0 / math.sqrt(nope + rope)

    hc = heads // chunks
    width = hc * (nope + rope)
    vm = pl.BlockSpec(memory_space=pltpu.VMEM)
    anyspec = pl.BlockSpec(memory_space=pl.ANY)
    big = (w_uk, w_uv, prefix_latent, prefix_rope, suffix_latent, suffix_rope)
    V = pltpu.VMEM
    D = pltpu.SemaphoreType.DMA
    scratch = [V(a.shape, a.dtype) for a in big] + [
        V((chunks, n, pr, width), BF16),
        V((chunks, n, pr, width), BF16),
        V((t, heads * share, latent), BF16),
        V((t, heads * share, latent), BF16),
        V((t, heads * share, latent), BF16),
        V((t, share, heads * rope), BF16),
        V((t, heads * share, rope), BF16),
        V((t, heads * share, latent), BF16),
        V((t, heads * share, latent), BF16),
        V((2 * share, 128), F32),
        V((t, 2 * share, 128), F32),
        V((chunks, n, pr, hc * value), BF16),
        V((chunks, n, pr, hc * value), BF16),
        V((own * n * cap, 128), F32),
        V((n, pr, 128), F32),
        V((n, pr, 128), F32),
        V((own * n * cap, hc * value), BF16),
        V((batch, heads * value), BF16),
        V((n * pr, batch), F32),
        V((heads * share, heads * share), BF16),
        V((heads * share, heads * share), BF16),
        V((own * n * cap, n * pr), BF16),
        V((n * pr, own * n * cap), BF16),
        V((heads * t, 128), F32),
        D((6,)), D((t,)), D((t,)), D((HALVES, t)), D((HALVES, t)), D((HALVES, t)), D((HALVES, t)), D((t,)), D((t,)),
        D((chunks, n)), D((chunks, n)), D((chunks, n)), D((chunks, n)), D((n,)), D((n,)),
    ]
    return pl.pallas_call(
        functools.partial(kernel, (n, t, chunks, cap, score_scale)),
        out_shape=jax.ShapeDtypeStruct((batch, heads * value), BF16),
        in_specs=[vm] * 3 + [pl.BlockSpec(memory_space=pltpu.SMEM)] * 2 + [anyspec] * 6,
        out_specs=vm,
        scratch_shapes=scratch,
        compiler_params=pltpu.CompilerParams(
            collective_id=0, has_side_effects=True, vmem_limit_bytes=63 * 1024 * 1024),
    )(q_nope, q_rope, request_prefix.reshape(1, -1), prefix_slot.reshape(1, -1), suffix_len, *big)


def solution(mesh):
    in_specs = (
        P("grp", "tp"),
        P("grp", "tp"),
        P("tp", None, None),
        P("tp", None, None),
        P("grp", None, None),
        P("grp", None, None),
        P(("grp", "tp"), None, None),
        P(("grp", "tp"), None, None),
        P("grp", None),
        P("grp"),
        P(),
    )
    return jax.shard_map(local, mesh=mesh, in_specs=in_specs, out_specs=P("grp", "tp"), check_vma=False)
```
